32 devices in a mesh: job: 2 (over x), tm: 2 (over core), rows: 8 (over z, y).
Axes of the slice: x: 2, y: 2, z: 4, core: 2. Of those that a mesh axis runs over, the one named last changes fastest.
Arguments:
- prior: bfloat16 [2, 524288, 64], P('tm', ('job', 'rows')), parts along dimension 1, may hold values from -80 to 80
- snapshots: bfloat16 [2, 524288, 256], P('tm', ('job', 'rows')), parts along dimension 1, may hold values from -60 to 60
Outputs:
- merged: bfloat16 [524288, 64], P(('job', 'rows'), 'tm'), parts along dimension 0
The draws below stay inside these ranges and needn't reach their ends.
There are 2 independent parts, one for each index of `job`. The reference program is written for one: setup_inputs(seed, part) draws one part's arguments, and reference() takes and returns one part's arrays. A program takes and returns all parts, laid end to end along the dimension named above; each array names one. Nothing has to cross between parts.
All inputs are finite; a program needn't handle non-finite values.
Results may differ from the reference program's by a relative error of at most 0.011.
Values may be sent and summed in bfloat16 or wider, within the bound.
No kernel may reach another device: no remote copies, remote signals or barrier semaphores. Data moves between devices by JAX's collectives and lax.ppermute only.
A program may use at most 128 MiB of HBM per device.

```python
import jax
import jax.numpy as jnp
from jax import lax

KEEP = 64
NEW = 64
STEPS = 4
ITERS = 2
DOFS = 262144
SNAPS = 256
N_TM = 2


def shared_fields(key):
    fields = 3 * KEEP + NEW
    key_u, key_r, key_s = jax.random.split(jax.random.fold_in(key, 5), 3)
    spatial = jnp.clip(jax.random.normal(key_u, (DOFS, fields), jnp.float32), -5.0, 5.0)
    row_scale = jnp.exp(jax.random.uniform(key_r, (DOFS, 1), jnp.float32, jnp.log(0.3), jnp.log(3.0)))
    ranks = jnp.arange(fields, dtype=jnp.float32)
    spectrum = 3.0 / (1.0 + ranks / 16.0)
    jitter = jnp.exp(jax.random.uniform(key_s, (fields,), jnp.float32, jnp.log(0.7), jnp.log(1.4)))
    return (spatial * row_scale * (spectrum * jitter)[None, :], row_scale)


def mixed_field(key, shape):
    return jnp.clip(jax.random.normal(key, shape, jnp.float32), -5.0, 5.0)


def draw_prior(key, part):
    scaled, row_scale = shared_fields(key)
    fields = scaled.shape[1]
    own = jax.random.fold_in(key, 11)
    key_m, key_n, key_c = jax.random.split(own, 3)
    mixing = mixed_field(key_m, (N_TM, fields, KEEP)) * 0.25
    col_scale = jnp.exp(jax.random.uniform(key_c, (N_TM, 1, KEEP), jnp.float32, jnp.log(0.5), jnp.log(2.0)))
    values = jnp.einsum('dr,trk->tdk', scaled, mixing, precision=jax.lax.Precision.HIGHEST)
    noise = 0.2 * mixed_field(key_n, (N_TM, DOFS, KEEP)) * row_scale[None]
    return jnp.clip((values + noise) * col_scale, -80.0, 80.0).astype(jnp.bfloat16)


def draw_snapshots(key, part):
    scaled, row_scale = shared_fields(key)
    fields = scaled.shape[1]
    own = jax.random.fold_in(key, 23)
    key_a, key_n, key_c = jax.random.split(own, 3)
    amplitude = mixed_field(key_a, (N_TM, fields, SNAPS)) * 0.3
    col_scale = jnp.exp(jax.random.uniform(key_c, (N_TM, 1, SNAPS), jnp.float32, jnp.log(0.5), jnp.log(2.0)))
    values = jnp.einsum('dr,trs->tds', scaled, amplitude, precision=jax.lax.Precision.HIGHEST)
    noise = 0.2 * mixed_field(key_n, (N_TM, DOFS, SNAPS)) * row_scale[None]
    values = values + noise
    return jnp.clip(values * col_scale, -60.0, 60.0).astype(jnp.bfloat16)


def setup_inputs(seed: int = 0, part: int = 0) -> dict:
    key_list = jax.random.split(jax.random.key(seed), 3)
    own_keys = jax.random.split(jax.random.fold_in(key_list[2], part), 3)
    return {
        "prior": draw_prior(jax.random.fold_in(jax.random.fold_in(key_list[2], part), 71), part),
        "snapshots": draw_snapshots(jax.random.fold_in(jax.random.fold_in(key_list[2], part), 71), part),
    }


def basis_of(gram, keep):
    order = gram.shape[0]
    basis = jnp.eye(order, keep, dtype=jnp.float32)
    for turn in range(ITERS):
        image = jnp.dot(gram, basis, precision=lax.Precision.HIGHEST)
        inner = jnp.dot(image.T, image, precision=lax.Precision.HIGHEST)
        lower = jnp.linalg.cholesky(inner)
        basis = jax.scipy.linalg.solve_triangular(lower, image.T, lower=True).T
    return basis

def reduce_pair(joined):
    gram = jnp.dot(joined.T, joined, precision=lax.Precision.HIGHEST)
    basis = basis_of(gram, KEEP)
    return jnp.dot(joined, basis, precision=lax.Precision.HIGHEST)

def reference(prior, snapshots):
    groups = []
    for group in range(N_TM):
        modes = prior[group].astype(jnp.float32)
        for step in range(STEPS):
            fresh = snapshots[group][:, step * NEW:(step + 1) * NEW].astype(jnp.float32)
            modes = reduce_pair(jnp.concatenate([modes, fresh], axis=1))
        groups.append(modes)
    while len(groups) > 1:
        groups = [reduce_pair(jnp.concatenate([groups[2 * pos], groups[2 * pos + 1]], axis=1)) for pos in range(len(groups) // 2)]
    return groups[0].astype(jnp.bfloat16)
```

```python
import functools

import jax
import jax.numpy as jnp
from jax import lax
from jax.experimental import pallas as pl
from jax.experimental.pallas import tpu as pltpu
from jax.sharding import PartitionSpec as P

STEPS = 4
ITERS = 2
F32 = jnp.float32
NN = (((1,), (0,)), ((), ()))
NT = (((1,), (1,)), ((), ()))
TN = (((0,), (0,)), ((), ()))
VMEM = pltpu.MemorySpace.VMEM


def dot(a, b, dims=NN):
    return lax.dot_general(
        a, b, dims, precision=lax.Precision.HIGHEST, preferred_element_type=F32
    )


def fast(a, b, dims=NN):
    return lax.dot_general(a, b, dims, preferred_element_type=F32)


def spread_lanes(row):
    return jnp.broadcast_to(row, (8, row.shape[1]))


def spread_cols(col, width):
    return jnp.broadcast_to(col, (col.shape[0], width))


def iota(shape, dim):
    return lax.broadcasted_iota(jnp.int32, shape, dim)


def inverse_factor(square):
    order, width = square.shape
    lane = iota((order, width), 1)
    eye = (lane == iota((order, width), 0)).astype(F32)
    joined = jnp.where(lane < order, eye, square)
    rows = [joined[8 * b : 8 * b + 8] for b in range(order // 8)]
    sub = iota((8, width), 0)
    done = []
    for b in range(order // 8):
        here = rows[b]
        first = order + 8 * b
        cols = [spread_cols(here[:, first + j : first + j + 1], width) for j in range(8)]
        below = [
            [spread_cols(rows[t][:, first + j : first + j + 1], width) for j in range(8)]
            for t in range(b + 1, order // 8)
        ]
        kept = jnp.zeros_like(here)
        for j in range(8):
            pivot = spread_lanes(cols[j][j : j + 1])
            inv = 1.0 / pivot
            scaled = spread_lanes(here[j : j + 1]) * inv
            kept = jnp.where(sub == j, here * lax.rsqrt(pivot), kept)
            here = jnp.where(sub == j, scaled, here - cols[j] * scaled)
            for k in range(j + 1, 8):
                part = spread_lanes(cols[k][j : j + 1]) * inv
                cols[k] = jnp.where(sub == j, part, cols[k] - cols[j] * part)
        done.append(kept)
        if b + 1 < order // 8:
            flat = [spread_lanes(here[j : j + 1]) for j in range(8)]
            for at, t in enumerate(range(b + 1, order // 8)):
                terms = [below[at][j] * flat[j] for j in range(8)]
                while len(terms) > 1:
                    terms = [terms[i] + terms[i + 1] for i in range(0, len(terms), 2)]
                rows[t] = rows[t] - terms[0]
    full = jnp.concatenate(done, axis=0)
    return jnp.where(lane < order, full, 0.0)


def basis_rows(gram, keep):
    image = gram[:keep]
    for turn in range(ITERS):
        twice = jnp.concatenate([image, image], axis=0)
        inner = dot(image, twice, NT)
        basis = dot(inverse_factor(inner), twice)
        if turn + 1 < ITERS:
            image = dot(basis, gram)
    return basis


def unpack(packed, keep):
    tile = lambda i: packed[:, 128 * i : 128 * i + 128]
    lane = iota((keep, 128), 1)
    zero = jnp.zeros((keep, 128), F32)
    upper = jnp.concatenate(
        [
            jnp.concatenate([tile(0), tile(1)], axis=1),
            jnp.concatenate([tile(6), tile(2)], axis=1),
            jnp.concatenate([zero, tile(3)], axis=1),
            jnp.concatenate([zero, tile(7)], axis=1),
        ],
        axis=0,
    )
    size = upper.shape[0]
    row_block = iota((size, size), 0) // keep
    col_block = iota((size, size), 1) // keep
    square = jnp.where(row_block <= col_block, upper, upper.T)
    cross = jnp.concatenate([tile(4), tile(5)], axis=1)
    corner = jnp.where(lane < keep, tile(6), 0.0)
    low = jnp.concatenate([cross, corner], axis=1)
    cross_pad = jnp.concatenate([cross, jnp.zeros_like(cross)], axis=0)
    top = jnp.concatenate([square, cross_pad.T], axis=1)
    return jnp.concatenate([top, low, jnp.zeros_like(low)], axis=0)


def steps_kernel(left_ref, right_ref, out_ref, total_ref, weights_ref):
    keep = left_ref.shape[0]
    total_ref[...] = unpack(left_ref[...] + right_ref[...], keep)
    width = total_ref.shape[0]
    frames = STEPS * keep
    shape = (keep, width)
    weights_ref[...] = (iota(shape, 1) == iota(shape, 0) + frames).astype(F32)

    @pl.loop(0, STEPS)
    def _(step):
        picker = (iota(shape, 1) == iota(shape, 0) + step * keep).astype(F32)
        coeffs = jnp.concatenate([weights_ref[...], picker], axis=0)
        gram = dot(dot(coeffs, total_ref[...]), coeffs, NT)
        weights_ref[...] = dot(basis_rows(gram, keep), coeffs)

    out_ref[...] = weights_ref[...]


def steps_weights(left, right, keep):
    width = (STEPS + 2) * keep
    return pl.pallas_call(
        steps_kernel,
        out_shape=jax.ShapeDtypeStruct((keep, width), F32),
        in_specs=[pl.BlockSpec(memory_space=VMEM)] * 2,
        out_specs=pl.BlockSpec(memory_space=VMEM),
        scratch_shapes=[pltpu.VMEM((width, width), F32), pltpu.VMEM((keep, width), F32)],
        name="steps",
    )(left, right)


def gram_kernel(prior_ref, frames_ref, out_ref, square_ref, cross_ref, corner_ref):
    step = pl.program_id(0)

    @pl.when(step == 0)
    def _():
        square_ref[...] = jnp.zeros_like(square_ref)
        cross_ref[...] = jnp.zeros_like(cross_ref)
        corner_ref[...] = jnp.zeros_like(corner_ref)

    prior = prior_ref[...]
    frames = frames_ref[...]
    square_ref[...] += fast(frames, frames, TN)
    cross_ref[...] += fast(prior, frames)
    corner_ref[...] += fast(prior, prior, NT)

    @pl.when(step == pl.num_programs(0) - 1)
    def _():
        keep = prior_ref.shape[0]
        square = square_ref[...]
        corner = corner_ref[...]
        wide = jnp.concatenate([corner, jnp.zeros_like(corner)], axis=1)
        lane = iota(wide.shape, 1)
        out_ref[:, 0:256] = square[0:64]
        out_ref[:, 256:384] = square[64:128, 128:256]
        out_ref[:, 384:512] = square[128:192, 128:256]
        out_ref[:, 512:768] = cross_ref[...]
        out_ref[:, 768:896] = jnp.where(lane < keep, wide, square[64:128, 0:128])
        out_ref[:, 896:1024] = square[192:256, 128:256]


def local_gram(prior_t, frames, chunk):
    keep, rows = prior_t.shape
    width = frames.shape[1]
    return pl.pallas_call(
        gram_kernel,
        grid=(rows // chunk,),
        out_shape=jax.ShapeDtypeStruct((keep, 16 * keep), F32),
        in_specs=[
            pl.BlockSpec((keep, chunk), lambda i: (0, i)),
            pl.BlockSpec((chunk, width), lambda i: (i, 0)),
        ],
        out_specs=pl.BlockSpec((keep, 16 * keep), lambda i: (0, 0)),
        scratch_shapes=[
            pltpu.VMEM((width, width), F32),
            pltpu.VMEM((keep, width), F32),
            pltpu.VMEM((keep, keep), F32),
        ],
        name="gram",
    )(prior_t, frames)


def split(value):
    high = value.astype(jnp.bfloat16)
    return high, (value - high.astype(F32)).astype(jnp.bfloat16)


def modes_kernel(weights_ref, prior_ref, frames_ref, out_ref):
    keep = prior_ref.shape[0]
    width = frames_ref.shape[1]
    both = jnp.concatenate(split(weights_ref[...]), axis=0)
    part = fast(both[:, :width], frames_ref[...], NT)
    part += fast(both[:, width : width + keep], prior_ref[...])
    out_ref[...] = (part[:keep] + part[keep:]).astype(out_ref.dtype)


def project(weights, prior_t, frames, chunk, first, count):
    keep, rows = prior_t.shape
    width = frames.shape[1]
    return pl.pallas_call(
        modes_kernel,
        grid=(count,),
        out_shape=jax.ShapeDtypeStruct((keep, count * chunk), jnp.bfloat16),
        in_specs=[
            pl.BlockSpec(weights.shape, lambda i: (0, 0)),
            pl.BlockSpec((keep, chunk), lambda i: (0, i + first)),
            pl.BlockSpec((chunk, width), lambda i: (i + first, 0)),
        ],
        out_specs=pl.BlockSpec((keep, chunk), lambda i: (0, i)),
        name="project",
    )(weights, prior_t, frames)


def pair_kernel(own_ref, other_ref, out_ref):
    @pl.when(pl.program_id(0) == 0)
    def _():
        out_ref[...] = jnp.zeros_like(out_ref)

    both = jnp.concatenate([own_ref[...], other_ref[...]], axis=0)
    out_ref[...] += fast(both, both, NT)


def pair_gram(own, other, chunk):
    keep, rows = own.shape
    block = pl.BlockSpec((keep, chunk), lambda i: (0, i))
    return pl.pallas_call(
        pair_kernel,
        grid=(rows // chunk,),
        out_shape=jax.ShapeDtypeStruct((2 * keep, 2 * keep), F32),
        in_specs=[block, block],
        out_specs=pl.BlockSpec((2 * keep, 2 * keep), lambda i: (0, 0)),
        name="pair",
    )(own, other)


def merge_kernel(index_ref, left_ref, right_ref, out_ref):
    gram = left_ref[...] + right_ref[...]
    keep = gram.shape[0] // 2
    first = index_ref[0] == 0
    swapped = pltpu.roll(pltpu.roll(gram, keep, 1), keep, 0)
    basis = basis_rows(jnp.where(first, gram, swapped), keep)
    half = out_ref.shape[0]
    out_ref[...] = jnp.where(first, basis[:half], pltpu.roll(basis[half:], keep, 1))


def merge_weights(index, left, right):
    order = left.shape[0]
    return pl.pallas_call(
        merge_kernel,
        out_shape=jax.ShapeDtypeStruct((order // 4, order), F32),
        in_specs=[pl.BlockSpec(memory_space=pltpu.MemorySpace.SMEM)]
        + [pl.BlockSpec(memory_space=VMEM)] * 2,
        out_specs=pl.BlockSpec(memory_space=VMEM),
        name="merge",
    )(index, left, right)


def output_kernel(weights_ref, own_ref, other_ref, out_ref):
    half = out_ref.shape[0]
    both = jnp.concatenate([own_ref[...], other_ref[...]], axis=0)
    part = fast(jnp.concatenate(split(weights_ref[...]), axis=0), both)
    out_ref[...] = (part[:half] + part[half:]).astype(out_ref.dtype)


def output(weights, own, other, chunk):
    keep, rows = own.shape
    block = pl.BlockSpec((keep, chunk), lambda i: (0, i))
    return pl.pallas_call(
        output_kernel,
        grid=(rows // chunk,),
        out_shape=jax.ShapeDtypeStruct((keep // 2, rows), jnp.bfloat16),
        in_specs=[pl.BlockSpec(weights.shape, lambda i: (0, 0)), block, block],
        out_specs=pl.BlockSpec((keep // 2, chunk), lambda i: (0, i)),
        name="output",
    )(weights, own, other)


def flip(block, axis, mask):
    count = lax.axis_size(axis)
    return lax.ppermute(block, axis, [(i, i ^ mask) for i in range(count)])


def all_but_last_sum(value, axis):
    count = lax.axis_size(axis)
    mask = 1
    while 2 * mask < count:
        value = value + flip(value, axis, mask)
        mask *= 2
    return value, flip(value, axis, mask)


def block_of(rows, limit):
    size = min(rows, limit)
    while rows % size:
        size //= 2
    return size


def shards(prior, snapshots):
    prior_t = prior[0].T
    frames = snapshots[0]
    keep, rows = prior_t.shape
    local = local_gram(prior_t, frames, block_of(rows, 8192))
    weights = steps_weights(*all_but_last_sum(local, "rows"), keep)
    own = project(weights, prior_t, frames, block_of(rows, 4096), 0, rows // block_of(rows, 4096))
    other = flip(own, "tm", 1)
    gram = pair_gram(own, other, block_of(rows, 8192))
    index = lax.axis_index("tm").astype(jnp.int32).reshape(1)
    final = merge_weights(index, *all_but_last_sum(gram, "rows"))
    return output(final, own, other, block_of(rows, 8192)).T


def solution(mesh):
    in_specs = (P("tm", ("job", "rows"), None), P("tm", ("job", "rows"), None))
    out_specs = P(("job", "rows"), "tm")
    return jax.shard_map(shards, mesh=mesh, in_specs=in_specs, out_specs=out_specs, check_vma=False)
```

```python
import functools

import jax
import jax.numpy as jnp
from jax import lax
from jax.experimental import pallas as pl
from jax.experimental.pallas import tpu as pltpu
from jax.sharding import PartitionSpec as P

STEPS = 4
ITERS = 2
F32 = jnp.float32
NN = (((1,), (0,)), ((), ()))
NT = (((1,), (1,)), ((), ()))
TN = (((0,), (0,)), ((), ()))
VMEM = pltpu.MemorySpace.VMEM
PIECES = 4
CHUNK = 4096
GRAM_MB, PROJ_MB, PAIR_MB, OUT_MB = 36, 12, 6, 8
OUTVM = pltpu.VMEM


def dot(a, b, dims=NN):
    return lax.dot_general(
        a, b, dims, precision=lax.Precision.HIGHEST, preferred_element_type=F32
    )


def fast(a, b, dims=NN):
    return lax.dot_general(a, b, dims, preferred_element_type=F32)


def spread_lanes(row):
    return jnp.broadcast_to(row, (8, row.shape[1]))


def spread_cols(col, width):
    return jnp.broadcast_to(col, (col.shape[0], width))


def grant(mebibytes):
    return pltpu.CompilerParams(vmem_limit_bytes=mebibytes << 20)


def iota(shape, dim):
    return lax.broadcasted_iota(jnp.int32, shape, dim)


def pair_sum(terms):
    while len(terms) > 1:
        terms = [a + b for a, b in zip(terms[::2], terms[1::2])]
    return terms[0]


def inverse_factor(square, zero):
    order, width = square.shape
    lane = iota((order, width), 1)
    eye = (lane == iota((order, width), 0)).astype(F32)
    joined = jnp.where(lane < order, eye, square)
    count = order // 8
    rows = [joined[8 * b : 8 * b + 8] for b in range(count)]
    sub = iota((8, width), 0)
    done = []
    for b in range(count):
        here = rows[b]
        first = order + 8 * b
        cols = [spread_cols(here[:, first + j : first + j + 1], width) + zero for j in range(8)]
        below = [
            [spread_cols(rows[t][:, first + j : first + j + 1], width) for t in range(b + 1, count)]
            for j in range(8)
        ]
        kept = here
        for j in range(0, 8, 2):
            left, right = cols[j], cols[j + 1]
            at_left, at_right = sub == j, sub == j + 1
            pp, pq, qq = (
                spread_lanes(left[j : j + 1]),
                spread_lanes(right[j : j + 1]),
                spread_lanes(right[j + 1 : j + 2]),
            )
            inv = 1.0 / (pp * qq - pq * pq)
            ipp, ipq, iqq = qq * inv, -pq * inv, pp * inv

            def solve(value):
                top, low = spread_lanes(value[j : j + 1]), spread_lanes(value[j + 1 : j + 2])
                up, down = ipp * top + ipq * low, ipq * top + iqq * low
                rest = value - (left * up + right * down)
                return top, low, jnp.where(at_left, up, jnp.where(at_right, down, rest))

            for k in range(j + 2, 8):
                cols[k] = solve(cols[k])[2]
            top, low, here = solve(here)
            scale = lax.rsqrt(pp)
            ratio = pq * scale
            unit = top * scale
            kept = jnp.where(at_left, unit, kept)
            kept = jnp.where(
                at_right, (low - ratio * unit) * lax.rsqrt(qq - ratio * ratio), kept
            )
        done.append(kept)
        if b + 1 < count:
            flat = [spread_lanes(here[j : j + 1]) for j in range(8)]
            for t in range(b + 1, count):
                rows[t] = rows[t] - pair_sum([below[j][t - b - 1] * flat[j] for j in range(8)])
    return jnp.where(lane < order, jnp.concatenate(done, axis=0), 0.0)


def basis_rows(gram, keep, zero):
    image = gram[:keep]
    for turn in range(ITERS):
        twice = jnp.concatenate([image, image], axis=0)
        inner = dot(image, twice, NT)
        basis = dot(inverse_factor(inner, zero), twice)
        if turn + 1 < ITERS:
            image = dot(basis, gram)
    return basis


def unpack(packed, keep):
    tile = lambda i: packed[:, 128 * i : 128 * i + 128]
    lane = iota((keep, 128), 1)
    zero = jnp.zeros((keep, 128), F32)
    upper = jnp.concatenate(
        [
            jnp.concatenate([tile(0), tile(1)], axis=1),
            jnp.concatenate([tile(6), tile(2)], axis=1),
            jnp.concatenate([zero, tile(3)], axis=1),
            jnp.concatenate([zero, tile(7)], axis=1),
        ],
        axis=0,
    )
    size = upper.shape[0]
    row_block = iota((size, size), 0) // keep
    col_block = iota((size, size), 1) // keep
    square = jnp.where(row_block <= col_block, upper, upper.T)
    cross = jnp.concatenate([tile(4), tile(5)], axis=1)
    corner = jnp.where(lane < keep, tile(6), 0.0)
    low = jnp.concatenate([cross, corner], axis=1)
    cross_pad = jnp.concatenate([cross, jnp.zeros_like(cross)], axis=0)
    top = jnp.concatenate([square, cross_pad.T], axis=1)
    return jnp.concatenate([top, low, jnp.zeros_like(low)], axis=0)


def unit_trace(gram):
    eye = iota(gram.shape, 0) == iota(gram.shape, 1)
    return gram / jnp.sum(jnp.where(eye, gram, 0.0))


def steps_kernel(left_ref, right_ref, out_ref, total_ref, both_ref, zero_ref):
    keep = left_ref.shape[0]
    zero_ref[...] = jnp.zeros_like(zero_ref)
    total = unit_trace(unpack(left_ref[...] + right_ref[...], keep))
    total_ref[...] = total
    width = total.shape[0]
    frames = STEPS * keep
    shape = (keep, width)
    both_ref[:keep, :width] = total[frames : frames + keep]
    both_ref[:keep, width:] = (iota(shape, 1) == iota(shape, 0) + frames).astype(F32)

    @pl.loop(0, STEPS)
    def _(step):
        at = pl.multiple_of(step * keep, keep)
        both_ref[keep:, :width] = total_ref[pl.ds(at, keep)]
        both_ref[keep:, width:] = (iota(shape, 1) == iota(shape, 0) + at).astype(F32)
        both = both_ref[...]
        gram = dot(both[:, :width], both[:, width:], NT)
        both_ref[:keep] = dot(basis_rows(gram, keep, zero_ref[...]), both)

    out_ref[...] = both_ref[:keep, width:]


def steps_weights(left, right, keep):
    width = (STEPS + 2) * keep
    return pl.pallas_call(
        steps_kernel,
        out_shape=jax.ShapeDtypeStruct((keep, width), F32),
        in_specs=[pl.BlockSpec(memory_space=VMEM)] * 2,
        out_specs=pl.BlockSpec(memory_space=VMEM),
        scratch_shapes=[
            pltpu.VMEM((width, width), F32),
            pltpu.VMEM((2 * keep, 2 * width), F32),
            pltpu.VMEM((8, 2 * keep), F32),
        ],
        name="steps",
        compiler_params=grant(6),
    )(left, right)


def gram_kernel(prior_in, frames_in, out_ref, prior_ref, frames_ref, sems, square_ref, corner_ref):
    keep, rows = prior_ref.shape
    width = frames_ref.shape[1]
    count = sems.shape[1]
    size = rows // count

    def copies(i):
        at = slice(i * size, i * size + size)
        return (
            pltpu.make_async_copy(prior_in.at[:, at], prior_ref.at[:, at], sems.at[0, i]),
            pltpu.make_async_copy(frames_in.at[at], frames_ref.at[at], sems.at[1, i]),
        )

    for i in range(count):
        for copy in copies(i):
            copy.start()
    for i in range(count):
        for copy in copies(i):
            copy.wait()
        at = slice(i * size, i * size + size)
        frames = frames_ref[at]
        prior = prior_ref[:, at]
        part = fast(jnp.concatenate([frames.T, prior], axis=0), frames)
        last = fast(prior, prior, NT)
        square_ref[...] = part if i == 0 else square_ref[...] + part
        corner_ref[...] = last if i == 0 else corner_ref[...] + last

    corner = corner_ref[...]
    wide = jnp.concatenate([corner, jnp.zeros_like(corner)], axis=1)
    lane = iota(wide.shape, 1)
    out_ref[:, 0:256] = square_ref[0:64]
    out_ref[:, 256:384] = square_ref[64:128, 128:256]
    out_ref[:, 384:512] = square_ref[128:192, 128:256]
    out_ref[:, 512:768] = square_ref[256:320]
    out_ref[:, 768:896] = jnp.where(lane < keep, wide, square_ref[64:128, 0:128])
    out_ref[:, 896:1024] = square_ref[192:256, 128:256]


def local_gram(prior_t, frames, size):
    keep, rows = prior_t.shape
    width = frames.shape[1]
    return pl.pallas_call(
        gram_kernel,
        out_shape=(
            jax.ShapeDtypeStruct((keep, 16 * keep), F32),
            OUTVM(prior_t.shape, prior_t.dtype),
            OUTVM(frames.shape, frames.dtype),
        ),
        in_specs=[pl.BlockSpec(memory_space=pltpu.MemorySpace.HBM)] * 2,
        out_specs=[pl.BlockSpec(memory_space=VMEM)] * 3,
        scratch_shapes=[
            pltpu.SemaphoreType.DMA((2, rows // size)),
            pltpu.VMEM((width + keep, width), F32),
            pltpu.VMEM((keep, keep), F32),
        ],
        name="gram",
        compiler_params=grant(GRAM_MB),
    )(prior_t, frames)


def split(value):
    high = value.astype(jnp.bfloat16)
    return high, (value - high.astype(F32)).astype(jnp.bfloat16)


def modes_kernel(first, weights_ref, prior_ref, frames_ref, out_ref):
    keep = prior_ref.shape[0]
    width = frames_ref.shape[1]
    rows = out_ref.shape[1]
    both = jnp.concatenate(split(weights_ref[:, : width + keep]), axis=0)
    size = block_of(rows, 2048)
    for at in range(0, rows, size):
        here = slice(first + at, first + at + size)
        whole = jnp.concatenate([frames_ref[here].T, prior_ref[:, here]], axis=0)
        part = fast(both, whole)
        out_ref[:, at : at + size] = (part[:keep] + part[keep:]).astype(out_ref.dtype)


def project(weights, prior_t, frames, first, rows):
    keep = prior_t.shape[0]
    return pl.pallas_call(
        functools.partial(modes_kernel, first),
        out_shape=OUTVM((keep, rows), jnp.bfloat16),
        in_specs=[pl.BlockSpec(memory_space=VMEM)] * 3,
        out_specs=pl.BlockSpec(memory_space=VMEM),
        name="project",
        compiler_params=grant(PROJ_MB),
    )(weights, prior_t, frames)


def pair_kernel(own_ref, other_ref, *rest):
    out_ref = rest[-1]
    both = jnp.concatenate([own_ref[...], other_ref[...]], axis=0)
    gram = fast(both, both, NT)
    out_ref[...] = rest[0][...] + gram if len(rest) > 1 else gram


def pair_gram(own, other, *sofar):
    keep = own.shape[0]
    return pl.pallas_call(
        pair_kernel,
        out_shape=jax.ShapeDtypeStruct((2 * keep, 2 * keep), F32),
        in_specs=[pl.BlockSpec(memory_space=VMEM)] * (2 + len(sofar)),
        out_specs=pl.BlockSpec(memory_space=VMEM),
        name="pair",
        compiler_params=grant(PAIR_MB),
    )(own, other, *sofar)


def merge_kernel(left_ref, right_ref, out_ref, zero_ref):
    zero_ref[...] = jnp.zeros_like(zero_ref)
    gram = unit_trace(left_ref[...] + right_ref[...])
    keep = gram.shape[0] // 2
    first = lax.axis_index("tm") == 0
    swapped = pltpu.roll(pltpu.roll(gram, keep, 1), keep, 0)
    basis = basis_rows(jnp.where(first, gram, swapped), keep, zero_ref[...])
    half = out_ref.shape[0]
    out_ref[...] = jnp.where(first, basis[:half], pltpu.roll(basis[half:], keep, 1))


def merge_weights(left, right):
    order = left.shape[0]
    return pl.pallas_call(
        merge_kernel,
        out_shape=jax.ShapeDtypeStruct((order // 4, order), F32),
        in_specs=[pl.BlockSpec(memory_space=VMEM)] * 2,
        out_specs=pl.BlockSpec(memory_space=VMEM),
        scratch_shapes=[pltpu.VMEM((8, order), F32)],
        name="merge",
        compiler_params=grant(2),
    )(left, right)


def output_kernel(pieces, weights_ref, *refs):
    owns, others = refs[:pieces], refs[pieces : 2 * pieces]
    out_ref, held_ref, sems = refs[2 * pieces :]
    half = out_ref.shape[0]
    weights = jnp.concatenate(split(weights_ref[...]), axis=0)
    rows = owns[0].shape[1]
    copies = []
    for i in range(pieces):
        both = jnp.concatenate([owns[i][...], others[i][...]], axis=0)
        part = fast(weights, both)
        here = slice(i * rows, i * rows + rows)
        held_ref[:, here] = (part[:half] + part[half:]).astype(out_ref.dtype)
        copies.append(pltpu.make_async_copy(held_ref.at[:, here], out_ref.at[:, here], sems.at[i]))
        copies[-1].start()
    for copy in copies:
        copy.wait()


def output(weights, owns, others):
    keep = owns[0].shape[0]
    rows = sum(own.shape[1] for own in owns)
    shape = (keep // 2, rows)
    return pl.pallas_call(
        functools.partial(output_kernel, len(owns)),
        out_shape=jax.ShapeDtypeStruct(shape, jnp.bfloat16),
        in_specs=[pl.BlockSpec(memory_space=VMEM)] * (1 + 2 * len(owns)),
        out_specs=pl.BlockSpec(memory_space=pltpu.MemorySpace.HBM),
        scratch_shapes=[pltpu.VMEM(shape, jnp.bfloat16), pltpu.SemaphoreType.DMA((len(owns),))],
        name="output",
        compiler_params=grant(OUT_MB),
    )(weights, *owns, *others)


def flip(block, axis, mask):
    count = lax.axis_size(axis)
    return lax.ppermute(block, axis, [(i, i ^ mask) for i in range(count)])


def all_but_last_sum(value, axis):
    count = lax.axis_size(axis)
    masks = [1] + [(1 << bit + 1) - 2 for bit in range(1, count.bit_length() - 1)]
    for mask in masks[:-1]:
        value = value + flip(value, axis, mask)
    return value, flip(value, axis, masks[-1])


def block_of(rows, limit):
    size = min(rows, limit)
    while rows % size:
        size //= 2
    return size


def shards(prior, snapshots):
    keep = prior.shape[2]
    local, prior_t, frames = local_gram(prior[0].T, snapshots[0], block_of(prior.shape[1], CHUNK))
    rows = frames.shape[0]
    weights = steps_weights(*all_but_last_sum(local, "rows"), keep)
    piece = rows // PIECES
    owns, others = [], []
    for i in range(PIECES):
        owns.append(project(weights, prior_t, frames, i * piece, piece))
        others.append(flip(owns[-1], "tm", 1))
    gram = pair_gram(owns[0], others[0])
    for own, other in zip(owns[1:], others[1:]):
        gram = pair_gram(own, other, gram)
    final = merge_weights(*all_but_last_sum(gram, "rows"))
    return output(final, owns, others).T


def solution(mesh):
    in_specs = (P("tm", ("job", "rows"), None), P("tm", ("job", "rows"), None))
    out_specs = P(("job", "rows"), "tm")
    return jax.shard_map(shards, mesh=mesh, in_specs=in_specs, out_specs=out_specs, check_vma=False)
```

```python
import functools

import jax
import jax.numpy as jnp
from jax import lax
from jax.experimental import pallas as pl
from jax.experimental.pallas import tpu as pltpu
from jax.sharding import PartitionSpec as P

STEPS = 4
ITERS = 2
F32 = jnp.float32
NN = (((1,), (0,)), ((), ()))
NT = (((1,), (1,)), ((), ()))
TN = (((0,), (0,)), ((), ()))
VMEM = pltpu.MemorySpace.VMEM
PIECES = 4
AHEAD = 2
GRAM_MB, PROJ_MB, PAIR_MB, OUT_MB = 36, 12, 6, 8


def dot(a, b, dims=NN):
    return lax.dot_general(
        a, b, dims, precision=lax.Precision.HIGHEST, preferred_element_type=F32
    )


def fast(a, b, dims=NN):
    return lax.dot_general(a, b, dims, preferred_element_type=F32)


def spread_lanes(row):
    return jnp.broadcast_to(row, (8, row.shape[1]))


def spread_cols(col, width):
    return jnp.broadcast_to(col, (col.shape[0], width))


def grant(mebibytes):
    return pltpu.CompilerParams(vmem_limit_bytes=mebibytes << 20)


def iota(shape, dim):
    return lax.broadcasted_iota(jnp.int32, shape, dim)


def pair_sum(terms):
    while len(terms) > 1:
        terms = [a + b for a, b in zip(terms[::2], terms[1::2])]
    return terms[0]


def inverse_factor(square, zero):
    order, width = square.shape
    lane = iota((order, width), 1)
    eye = (lane == iota((order, width), 0)).astype(F32)
    joined = jnp.where(lane < order, eye, square)
    count = order // 8
    rows = [joined[8 * b : 8 * b + 8] for b in range(count)]
    sub = iota((8, width), 0)
    done = []
    for b in range(count):
        here = rows[b]
        first = order + 8 * b
        cols = [spread_cols(here[:, first + j : first + j + 1], width) + zero for j in range(8)]
        below = [
            [spread_cols(rows[t][:, first + j : first + j + 1], width) for t in range(b + 1, count)]
            for j in range(8)
        ]
        kept = here
        for j in range(0, 8, 2):
            left, right = cols[j], cols[j + 1]
            at_left, at_right = sub == j, sub == j + 1
            pp, pq, qq = (
                spread_lanes(left[j : j + 1]),
                spread_lanes(right[j : j + 1]),
                spread_lanes(right[j + 1 : j + 2]),
            )
            inv = 1.0 / (pp * qq - pq * pq)
            ipp, ipq, iqq = qq * inv, -pq * inv, pp * inv

            def solve(value):
                top, low = spread_lanes(value[j : j + 1]), spread_lanes(value[j + 1 : j + 2])
                up, down = ipp * top + ipq * low, ipq * top + iqq * low
                rest = value - (left * up + right * down)
                return top, low, jnp.where(at_left, up, jnp.where(at_right, down, rest))

            for k in range(j + 2, 8):
                cols[k] = solve(cols[k])[2]
            top, low, here = solve(here)
            scale = lax.rsqrt(pp)
            ratio = pq * scale
            unit = top * scale
            kept = jnp.where(at_left, unit, kept)
            kept = jnp.where(
                at_right, (low - ratio * unit) * lax.rsqrt(qq - ratio * ratio), kept
            )
        done.append(kept)
        if b + 1 < count:
            flat = [spread_lanes(here[j : j + 1]) for j in range(8)]
            for t in range(b + 1, count):
                rows[t] = rows[t] - pair_sum([below[j][t - b - 1] * flat[j] for j in range(8)])
    return jnp.where(lane < order, jnp.concatenate(done, axis=0), 0.0)


def basis_rows(gram, keep, zero):
    image = gram[:keep]
    for turn in range(ITERS):
        twice = jnp.concatenate([image, image], axis=0)
        inner = dot(image, twice, NT)
        basis = dot(inverse_factor(inner, zero), twice)
        if turn + 1 < ITERS:
            image = dot(basis, gram)
    return basis


def unpack(packed, keep):
    tile = lambda i: packed[:, 128 * i : 128 * i + 128]
    lane, row = iota((keep, 128), 1), iota((keep, 128), 0)
    zero = jnp.zeros((keep, 128), F32)
    mixed = tile(6)
    diag = jnp.where(
        lane == 127,
        pltpu.roll(jnp.broadcast_to(mixed[keep - 2 : keep - 1], mixed.shape), 127, 1),
        pltpu.roll(jnp.broadcast_to(mixed[keep - 1 : keep], mixed.shape), keep, 1),
    )
    end = jnp.where(lane == row + keep, diag, pltpu.roll(tile(0), keep, 1))
    upper = jnp.concatenate(
        [
            jnp.concatenate([tile(0), tile(1)], axis=1),
            jnp.concatenate([mixed, tile(2)], axis=1),
            jnp.concatenate([zero, tile(3)], axis=1),
            jnp.concatenate([zero, end], axis=1),
        ],
        axis=0,
    )
    size = upper.shape[0]
    high, wide = iota((size, size), 0), iota((size, size), 1)
    last = size - keep
    held = ((high <= wide) & (wide < last)) | ((high < last) & (wide >= last))
    held |= (high >= wide) & (high >= last) & (wide >= last)
    square = jnp.where(held, upper, upper.T)
    cross = jnp.concatenate([tile(4), tile(5)], axis=1)
    turned = jnp.concatenate([mixed, mixed], axis=0).T[:keep]
    corner = jnp.where(lane < keep, jnp.where(row <= lane, mixed, turned), 0.0)
    low = jnp.concatenate([cross, corner], axis=1)
    cross_pad = jnp.concatenate([cross, jnp.zeros_like(cross)], axis=0)
    top = jnp.concatenate([square, cross_pad.T], axis=1)
    return jnp.concatenate([top, low, jnp.zeros_like(low)], axis=0)


def trace(gram):
    return jnp.sum(jnp.where(iota(gram.shape, 0) == iota(gram.shape, 1), gram, 0.0))


def steps_kernel(left_ref, right_ref, out_ref, modes_ref, total_ref, both_ref, zero_ref):
    keep = left_ref.shape[0]
    zero_ref[...] = jnp.zeros_like(zero_ref)
    total = unpack(left_ref[...] + right_ref[...], keep)
    scale = trace(total)
    total = total * (1.0 / scale)
    total_ref[...] = total
    width = total.shape[0]
    frames = STEPS * keep
    shape = (keep, width)
    both_ref[:keep, :width] = total[frames : frames + keep]
    both_ref[:keep, width:] = (iota(shape, 1) == iota(shape, 0) + frames).astype(F32)

    @pl.loop(0, STEPS)
    def _(step):
        at = pl.multiple_of(step * keep, keep)
        both_ref[keep:, :width] = total_ref[pl.ds(at, keep)]
        both_ref[keep:, width:] = (iota(shape, 1) == iota(shape, 0) + at).astype(F32)
        both = both_ref[...]
        gram = dot(both[:, :width], both[:, width:], NT)
        both_ref[:keep] = dot(basis_rows(gram, keep, zero_ref[...]), both)

    out_ref[...] = both_ref[:keep, width:]
    modes_ref[...] = dot(both_ref[:keep, :width], both_ref[:keep, width:], NT) * scale


def steps_weights(left, right, keep):
    width = (STEPS + 2) * keep
    return pl.pallas_call(
        steps_kernel,
        out_shape=(
            jax.ShapeDtypeStruct((keep, width), F32),
            jax.ShapeDtypeStruct((keep, keep), F32),
        ),
        in_specs=[pl.BlockSpec(memory_space=VMEM)] * 2,
        out_specs=[pl.BlockSpec(memory_space=VMEM)] * 2,
        scratch_shapes=[
            pltpu.VMEM((width, width), F32),
            pltpu.VMEM((2 * keep, 2 * width), F32),
            pltpu.VMEM((8, 2 * keep), F32),
        ],
        name="steps",
        compiler_params=grant(6),
    )(left, right)


def gram_kernel(cuts, prior_in, frames_in, out_ref, prior_ref, frames_ref, sems, square_ref, corner_ref):
    keep = prior_ref.shape[0]
    blocks = [slice(low, high) for low, high in zip(cuts[:-1], cuts[1:])]

    def copies(i):
        at = blocks[i]
        return (
            pltpu.make_async_copy(prior_in.at[:, at], prior_ref.at[:, at], sems.at[0, i]),
            pltpu.make_async_copy(frames_in.at[at], frames_ref.at[at], sems.at[1, i]),
        )

    for i in range(min(AHEAD, len(blocks))):
        for copy in copies(i):
            copy.start()
    for i, at in enumerate(blocks):
        for copy in copies(i):
            copy.wait()
        if i + AHEAD < len(blocks):
            for copy in copies(i + AHEAD):
                copy.start()
        frames = frames_ref[at]
        prior = prior_ref[:, at]
        part = jnp.concatenate([fast(frames, frames, TN), fast(prior, frames)], axis=0)
        last = fast(prior, prior, NT)
        square_ref[...] = part if i == 0 else square_ref[...] + part
        corner_ref[...] = last if i == 0 else corner_ref[...] + last

    corner = corner_ref[...]
    wide = jnp.concatenate([corner, jnp.zeros_like(corner)], axis=1)
    lane, row = iota(wide.shape, 1), iota(wide.shape, 0)
    end = square_ref[192:256, 128:256]
    diag = jnp.sum(jnp.where(lane == row + keep, end, 0.0), axis=0, keepdims=True)
    diag = jnp.broadcast_to(diag, end.shape)
    mixed = jnp.where(lane < keep, wide, square_ref[64:128, 0:128])
    mixed = jnp.where((row == keep - 1) & (lane < keep - 1), pltpu.roll(diag, keep, 1), mixed)
    mixed = jnp.where((row == keep - 2) & (lane == 0), pltpu.roll(diag, 1, 1), mixed)
    free = (lane < keep) & (row > lane)
    out_ref[:, 0:128] = jnp.where(free, pltpu.roll(end, keep, 1), square_ref[0:64, 0:128])
    out_ref[:, 128:256] = square_ref[0:64, 128:256]
    out_ref[:, 256:384] = square_ref[64:128, 128:256]
    out_ref[:, 384:512] = square_ref[128:192, 128:256]
    out_ref[:, 512:768] = square_ref[256:320]
    out_ref[:, 768:896] = mixed


def local_gram(prior_t, frames, cuts):
    keep, rows = prior_t.shape
    width = frames.shape[1]
    return pl.pallas_call(
        functools.partial(gram_kernel, cuts),
        out_shape=(
            jax.ShapeDtypeStruct((keep, 14 * keep), F32),
            pltpu.VMEM(prior_t.shape, prior_t.dtype),
            pltpu.VMEM(frames.shape, frames.dtype),
        ),
        in_specs=[pl.BlockSpec(memory_space=pltpu.MemorySpace.HBM)] * 2,
        out_specs=[pl.BlockSpec(memory_space=VMEM)] * 3,
        scratch_shapes=[
            pltpu.SemaphoreType.DMA((2, len(cuts) - 1)),
            pltpu.VMEM((width + keep, width), F32),
            pltpu.VMEM((keep, keep), F32),
        ],
        name="gram",
        compiler_params=grant(GRAM_MB),
    )(prior_t, frames)


def split(value):
    high = value.astype(jnp.bfloat16)
    return high, (value - high.astype(F32)).astype(jnp.bfloat16)


def modes_kernel(first, weights_ref, prior_ref, frames_ref, out_ref):
    keep = prior_ref.shape[0]
    width = frames_ref.shape[1]
    rows = out_ref.shape[1]
    both = jnp.concatenate(split(weights_ref[:, : width + keep]), axis=0)
    size = block_of(rows, 2048)
    for at in range(0, rows, size):
        here = slice(first + at, first + at + size)
        whole = jnp.concatenate([frames_ref[here].T, prior_ref[:, here]], axis=0)
        part = fast(both, whole)
        out_ref[:, at : at + size] = (part[:keep] + part[keep:]).astype(out_ref.dtype)


def project(weights, prior_t, frames, first, rows):
    keep = prior_t.shape[0]
    return pl.pallas_call(
        functools.partial(modes_kernel, first),
        out_shape=pltpu.VMEM((keep, rows), jnp.bfloat16),
        in_specs=[pl.BlockSpec(memory_space=VMEM)] * 3,
        out_specs=pl.BlockSpec(memory_space=VMEM),
        name="project",
        compiler_params=grant(PROJ_MB),
    )(weights, prior_t, frames)


def pair_kernel(own_ref, other_ref, *rest):
    out_ref = rest[-1]
    half = out_ref.shape[0]
    gram = fast(own_ref[...], other_ref[...], NT)
    gram = jnp.concatenate([gram[:half], gram[half:]], axis=1)
    out_ref[...] = rest[0][...] + gram if len(rest) > 1 else gram


def pair_gram(own, other, *sofar):
    keep = own.shape[0]
    return pl.pallas_call(
        pair_kernel,
        out_shape=jax.ShapeDtypeStruct((keep // 2, 2 * keep), F32),
        in_specs=[pl.BlockSpec(memory_space=VMEM)] * (2 + len(sofar)),
        out_specs=pl.BlockSpec(memory_space=VMEM),
        name="pair",
        compiler_params=grant(PAIR_MB),
    )(own, other, *sofar)


def merge_kernel(left_ref, right_ref, own_ref, other_ref, out_ref, zero_ref):
    zero_ref[...] = jnp.zeros_like(zero_ref)
    keep = own_ref.shape[0]
    halves = left_ref[...] + right_ref[...]
    cross = jnp.concatenate([halves[:, :keep], halves[:, keep:]], axis=0)
    gram = jnp.concatenate(
        [
            jnp.concatenate([own_ref[...], cross], axis=1),
            jnp.concatenate([cross.T, other_ref[...]], axis=1),
        ],
        axis=0,
    )
    gram = gram * (1.0 / trace(gram))
    first = lax.axis_index("tm") == 0
    swapped = pltpu.roll(pltpu.roll(gram, keep, 1), keep, 0)
    basis = basis_rows(jnp.where(first, gram, swapped), keep, zero_ref[...])
    half = out_ref.shape[0]
    out_ref[...] = jnp.where(first, basis[:half], pltpu.roll(basis[half:], keep, 1))


def merge_weights(left, right, own, other):
    keep = own.shape[0]
    return pl.pallas_call(
        merge_kernel,
        out_shape=jax.ShapeDtypeStruct((keep // 2, 2 * keep), F32),
        in_specs=[pl.BlockSpec(memory_space=VMEM)] * 4,
        out_specs=pl.BlockSpec(memory_space=VMEM),
        scratch_shapes=[pltpu.VMEM((8, 2 * keep), F32)],
        name="merge",
        compiler_params=grant(2),
    )(left, right, own, other)


def output_kernel(pieces, weights_ref, *refs):
    owns, others = refs[:pieces], refs[pieces : 2 * pieces]
    out_ref, held_ref, sems = refs[2 * pieces :]
    half = out_ref.shape[0]
    weights = jnp.concatenate(split(weights_ref[...]), axis=0)
    rows = owns[0].shape[1]
    copies = []
    for i in range(pieces):
        both = jnp.concatenate([owns[i][...], others[i][...]], axis=0)
        part = fast(weights, both)
        here = slice(i * rows, i * rows + rows)
        held_ref[:, here] = (part[:half] + part[half:]).astype(out_ref.dtype)
        copies.append(pltpu.make_async_copy(held_ref.at[:, here], out_ref.at[:, here], sems.at[i]))
        copies[-1].start()
    for copy in copies:
        copy.wait()


def output(weights, owns, others):
    keep = owns[0].shape[0]
    rows = sum(own.shape[1] for own in owns)
    shape = (keep // 2, rows)
    return pl.pallas_call(
        functools.partial(output_kernel, len(owns)),
        out_shape=jax.ShapeDtypeStruct(shape, jnp.bfloat16),
        in_specs=[pl.BlockSpec(memory_space=VMEM)] * (1 + 2 * len(owns)),
        out_specs=pl.BlockSpec(memory_space=pltpu.MemorySpace.HBM),
        scratch_shapes=[pltpu.VMEM(shape, jnp.bfloat16), pltpu.SemaphoreType.DMA((len(owns),))],
        name="output",
        compiler_params=grant(OUT_MB),
    )(weights, *owns, *others)


def flip(block, axis, mask):
    count = lax.axis_size(axis)
    return lax.ppermute(block, axis, [(i, i ^ mask) for i in range(count)])


def all_but_last_sum(value, axis, mirror):
    count = lax.axis_size(axis)
    masks = [1 << bit for bit in range(count.bit_length() - 1)]
    if mirror:
        masks = masks[:1] + [2 * mask - 2 for mask in masks[1:]]
    for mask in masks[:-1]:
        value = value + flip(value, axis, mask)
    return value, flip(value, axis, masks[-1])


def cuts_of(rows):
    unit = rows // 32
    return [unit * at for at in (0, 1, 4, 12, 20, 28, 32)]


def block_of(rows, limit):
    size = min(rows, limit)
    while rows % size:
        size //= 2
    return size


def shards(prior, snapshots):
    keep = prior.shape[2]
    rows = prior.shape[1]
    local, prior_t, frames = local_gram(prior[0].T, snapshots[0], cuts_of(rows))
    weights, own_gram = steps_weights(*all_but_last_sum(local, "rows", True), keep)
    other_gram = flip(own_gram, "tm", 1)
    piece = rows // PIECES
    owns, others = [], []
    for i in range(PIECES):
        owns.append(project(weights, prior_t, frames, i * piece, piece))
        others.append(flip(owns[-1], "tm", 1))
    cross = pair_gram(owns[0], others[0])
    for own, other in zip(owns[1:], others[1:]):
        cross = pair_gram(own, other, cross)
    final = merge_weights(*all_but_last_sum(cross, "rows", False), own_gram, other_gram)
    return output(final, owns, others).T


def solution(mesh):
    in_specs = (P("tm", ("job", "rows"), None), P("tm", ("job", "rows"), None))
    out_specs = P(("job", "rows"), "tm")
    return jax.shard_map(shards, mesh=mesh, in_specs=in_specs, out_specs=out_specs, check_vma=False)
```

```python
import functools

import jax
import jax.numpy as jnp
from jax import lax
from jax.experimental import pallas as pl
from jax.experimental.pallas import tpu as pltpu
from jax.sharding import PartitionSpec as P

STEPS = 4
ITERS = 2
F32 = jnp.float32
NN = (((1,), (0,)), ((), ()))
NT = (((1,), (1,)), ((), ()))
TN = (((0,), (0,)), ((), ()))
VMEM = pltpu.MemorySpace.VMEM
EARLY = 2
STEPS_FLOPS = 10**10
PIECES = 4
AHEAD = 2
GRAM_MB, PROJ_MB, PAIR_MB, OUT_MB = 36, 12, 6, 8


def dot(a, b, dims=NN):
    return lax.dot_general(
        a, b, dims, precision=lax.Precision.HIGHEST, preferred_element_type=F32
    )


def fast(a, b, dims=NN):
    return lax.dot_general(a, b, dims, preferred_element_type=F32)


def spread_lanes(row):
    return jnp.broadcast_to(row, (8, row.shape[1]))


def spread_cols(col, width):
    return jnp.broadcast_to(col, (col.shape[0], width))


def grant(mebibytes):
    return pltpu.CompilerParams(vmem_limit_bytes=mebibytes << 20)


def iota(shape, dim):
    return lax.broadcasted_iota(jnp.int32, shape, dim)


def pair_sum(terms):
    while len(terms) > 1:
        terms = [a + b for a, b in zip(terms[::2], terms[1::2])]
    return terms[0]


def eliminate(here, cols):
    cols = list(cols)
    sub = iota(here.shape, 0)
    kept = here
    for j in range(0, 8, 2):
        left, right = cols[j], cols[j + 1]
        at_left, at_right = sub == j, sub == j + 1
        pp, pq, qq = (
            spread_lanes(left[j : j + 1]),
            spread_lanes(right[j : j + 1]),
            spread_lanes(right[j + 1 : j + 2]),
        )
        inv = 1.0 / (pp * qq - pq * pq)
        ipp, ipq, iqq = qq * inv, -pq * inv, pp * inv

        def solve(value):
            top, low = spread_lanes(value[j : j + 1]), spread_lanes(value[j + 1 : j + 2])
            up, down = ipp * top + ipq * low, ipq * top + iqq * low
            rest = value - (left * up + right * down)
            return top, low, jnp.where(at_left, up, jnp.where(at_right, down, rest))

        for k in range(j + 2, len(cols)):
            cols[k] = solve(cols[k])[2]
        top, low, here = solve(here)
        scale = lax.rsqrt(pp)
        ratio = pq * scale
        unit = top * scale
        kept = jnp.where(at_left, unit, kept)
        kept = jnp.where(at_right, (low - ratio * unit) * lax.rsqrt(qq - ratio * ratio), kept)
    return kept, here, cols


def subtract(value, cols, rows):
    return value - pair_sum([col * row for col, row in zip(cols, rows)])


def inverse_factor(square, zero):
    order, width = square.shape
    lane = iota((order, width), 1)
    eye = (lane == iota((order, width), 0)).astype(F32)
    joined = jnp.where(lane < order, eye, square)
    count = order // 8
    rows = [joined[8 * b : 8 * b + 8] for b in range(count)]

    def columns(row, first):
        return [
            spread_cols(row[:, first + j : first + j + 1], width) + zero for j in range(16)
        ]

    def spread_rows(value):
        return [spread_lanes(value[j : j + 1]) for j in range(8)]

    done = []
    for b in range(0, count, 2):
        first = order + 8 * b
        cols, low_cols = columns(rows[b], first), columns(rows[b + 1], first)
        below = [columns(rows[t], first) for t in range(b + 2, count)]
        kept, high, cols = eliminate(rows[b], cols)
        done.append(kept)
        low = subtract(rows[b + 1], low_cols[:8], spread_rows(high))
        next_cols = [
            subtract(low_cols[k], low_cols[:8], spread_rows(cols[k])) for k in range(8, 16)
        ]
        kept, low, _ = eliminate(low, next_cols)
        done.append(kept)
        if b + 2 < count:
            low_rows = spread_rows(low)
            high_rows = spread_rows(subtract(high, cols[8:], low_rows))
            for at, t in enumerate(range(b + 2, count)):
                rows[t] = subtract(rows[t], below[at], high_rows + low_rows)
    return jnp.where(lane < order, jnp.concatenate(done, axis=0), 0.0)


def basis_rows(gram, keep, zero):
    image = gram[:keep]
    for turn in range(ITERS):
        twice = jnp.concatenate([image, image], axis=0)
        inner = dot(image, twice, NT)
        basis = dot(inverse_factor(inner, zero), twice)
        if turn + 1 < ITERS:
            image = dot(basis, gram)
    return basis


def assemble(square, cross, corner):
    low = jnp.concatenate([cross, corner], axis=1)
    size = square.shape[0]
    pad = jnp.zeros((128 - cross.shape[0], size), F32)
    top = jnp.concatenate([square, jnp.concatenate([cross, pad], axis=0).T], axis=1)
    return jnp.concatenate([top, low, jnp.zeros_like(low)], axis=0)


def prior_block(mixed):
    keep = mixed.shape[0]
    lane, row = iota(mixed.shape, 1), iota(mixed.shape, 0)
    turned = jnp.concatenate([mixed, mixed], axis=0).T[:keep]
    return jnp.where(lane < keep, jnp.where(row <= lane, mixed, turned), 0.0)


def unpack_early(early):
    mixed = early[:, 256:384]
    upper = jnp.concatenate([early[:, 0:128], mixed], axis=0)
    square = jnp.where(iota(upper.shape, 0) <= iota(upper.shape, 1), upper, upper.T)
    return assemble(square, early[:, 128:256], prior_block(mixed))


def unpack(early, late):
    keep = early.shape[0]
    tile = lambda i: late[:, 128 * i : 128 * i + 128]
    lane, row = iota((keep, 128), 1), iota((keep, 128), 0)
    zero = jnp.zeros((keep, 128), F32)
    first, mixed = early[:, 0:128], early[:, 256:384]
    diag = jnp.where(
        lane == 127,
        pltpu.roll(jnp.broadcast_to(mixed[keep - 2 : keep - 1], mixed.shape), 127, 1),
        pltpu.roll(jnp.broadcast_to(mixed[keep - 1 : keep], mixed.shape), keep, 1),
    )
    end = jnp.where(lane == row + keep, diag, pltpu.roll(first, keep, 1))
    upper = jnp.concatenate(
        [
            jnp.concatenate([first, tile(0)], axis=1),
            jnp.concatenate([mixed, tile(1)], axis=1),
            jnp.concatenate([zero, tile(2)], axis=1),
            jnp.concatenate([zero, end], axis=1),
        ],
        axis=0,
    )
    size = upper.shape[0]
    high, wide = iota((size, size), 0), iota((size, size), 1)
    last = size - keep
    held = ((high <= wide) & (wide < last)) | ((high < last) & (wide >= last))
    held |= (high >= wide) & (high >= last) & (wide >= last)
    square = jnp.where(held, upper, upper.T)
    cross = jnp.concatenate([early[:, 128:256], tile(3)], axis=1)
    return assemble(square, cross, prior_block(mixed))


def trace(gram):
    return jnp.sum(jnp.where(iota(gram.shape, 0) == iota(gram.shape, 1), gram, 0.0))


def run_steps(first, last, keep, total_ref, both_ref, zero):
    width = total_ref.shape[0]
    shape = (keep, width)

    @pl.loop(first, last)
    def _(step):
        at = pl.multiple_of(step * keep, keep)
        both_ref[keep:, :width] = total_ref[pl.ds(at, keep)]
        both_ref[keep:, width:] = (iota(shape, 1) == iota(shape, 0) + at).astype(F32)
        both = both_ref[...]
        gram = dot(both[:, :width], both[:, width:], NT)
        both_ref[:keep] = dot(basis_rows(gram, keep, zero), both)


def early_kernel(left_ref, right_ref, out_ref, total_ref, both_ref, zero_ref):
    keep = left_ref.shape[0]
    zero_ref[...] = jnp.zeros_like(zero_ref)
    total = unpack_early(left_ref[...] + right_ref[...])
    total = total * (1.0 / trace(total))
    total_ref[...] = total
    width = total.shape[0]
    frames = EARLY * keep
    shape = (keep, width)
    both_ref[:keep, :width] = total[frames : frames + keep]
    both_ref[:keep, width:] = (iota(shape, 1) == iota(shape, 0) + frames).astype(F32)
    run_steps(0, EARLY, keep, total_ref, both_ref, zero_ref[...])
    out_ref[...] = both_ref[:keep, width:]


def late_kernel(
    left_ref, right_ref, late_left, late_right, before_ref, out_ref, modes_ref, total_ref, both_ref, zero_ref
):
    keep = left_ref.shape[0]
    zero_ref[...] = jnp.zeros_like(zero_ref)
    total = unpack(left_ref[...] + right_ref[...], late_left[...] + late_right[...])
    scale = trace(total)
    total = total * (1.0 / scale)
    total_ref[...] = total
    width = total.shape[0]
    before = before_ref[...]
    fresh = EARLY * keep
    gap = jnp.zeros((keep, (STEPS - EARLY) * keep), F32)
    weights = jnp.concatenate([before[:, :fresh], gap, before[:, fresh:]], axis=1)
    both_ref[:keep, :width] = dot(weights, total)
    both_ref[:keep, width:] = weights
    run_steps(EARLY, STEPS, keep, total_ref, both_ref, zero_ref[...])
    out_ref[...] = both_ref[:keep, width:]
    modes_ref[...] = dot(both_ref[:keep, :width], both_ref[:keep, width:], NT) * scale


def steps_weights(early, late, keep):
    def call(kernel, shapes, width, *args):
        return pl.pallas_call(
            kernel,
            out_shape=tuple(jax.ShapeDtypeStruct(shape, F32) for shape in shapes),
            in_specs=[pl.BlockSpec(memory_space=VMEM)] * len(args),
            out_specs=tuple(pl.BlockSpec(memory_space=VMEM) for shape in shapes),
            scratch_shapes=[
                pltpu.VMEM((width, width), F32),
                pltpu.VMEM((2 * keep, 2 * width), F32),
                pltpu.VMEM((8, 2 * keep), F32),
            ],
            name="steps",
            compiler_params=grant(6),
            cost_estimate=pl.CostEstimate(
                flops=STEPS_FLOPS, bytes_accessed=1 << 20, transcendentals=0
            ),
        )(*args)

    (before,) = call(early_kernel, [(keep, (EARLY + 2) * keep)], (EARLY + 2) * keep, *early)
    width = (STEPS + 2) * keep
    return call(late_kernel, [(keep, width), (keep, keep)], width, *early, *late, before)


def gram_kernel(
    cuts, prior_in, frames_in, early_ref, late_ref, prior_ref, frames_ref, sems, square_ref, corner_ref
):
    keep = prior_ref.shape[0]
    blocks = [slice(low, high) for low, high in zip(cuts[:-1], cuts[1:])]

    def copies(i):
        at = blocks[i]
        return (
            pltpu.make_async_copy(prior_in.at[:, at], prior_ref.at[:, at], sems.at[0, i]),
            pltpu.make_async_copy(frames_in.at[at], frames_ref.at[at], sems.at[1, i]),
        )

    for i in range(min(AHEAD, len(blocks))):
        for copy in copies(i):
            copy.start()
    for i, at in enumerate(blocks):
        for copy in copies(i):
            copy.wait()
        if i + AHEAD < len(blocks):
            for copy in copies(i + AHEAD):
                copy.start()
        frames = frames_ref[at]
        prior = prior_ref[:, at]
        part = jnp.concatenate([fast(frames, frames, TN), fast(prior, frames)], axis=0)
        last = fast(prior, prior, NT)
        square_ref[...] = part if i == 0 else square_ref[...] + part
        corner_ref[...] = last if i == 0 else corner_ref[...] + last

    corner = corner_ref[...]
    wide = jnp.concatenate([corner, jnp.zeros_like(corner)], axis=1)
    lane, row = iota(wide.shape, 1), iota(wide.shape, 0)
    end = square_ref[192:256, 128:256]
    diag = jnp.sum(jnp.where(lane == row + keep, end, 0.0), axis=0, keepdims=True)
    diag = jnp.broadcast_to(diag, end.shape)
    mixed = jnp.where(lane < keep, wide, square_ref[64:128, 0:128])
    mixed = jnp.where((row == keep - 1) & (lane < keep - 1), pltpu.roll(diag, keep, 1), mixed)
    mixed = jnp.where((row == keep - 2) & (lane == 0), pltpu.roll(diag, 1, 1), mixed)
    free = (lane < keep) & (row > lane)
    early_ref[:, 0:128] = jnp.where(free, pltpu.roll(end, keep, 1), square_ref[0:64, 0:128])
    early_ref[:, 128:256] = square_ref[256:320, 0:128]
    early_ref[:, 256:384] = mixed
    late_ref[:, 0:128] = square_ref[0:64, 128:256]
    late_ref[:, 128:256] = square_ref[64:128, 128:256]
    late_ref[:, 256:384] = square_ref[128:192, 128:256]
    late_ref[:, 384:512] = square_ref[256:320, 128:256]


def local_gram(prior_t, frames, cuts):
    keep, rows = prior_t.shape
    width = frames.shape[1]
    return pl.pallas_call(
        functools.partial(gram_kernel, cuts),
        out_shape=(
            pltpu.VMEM((keep, 6 * keep), F32),
            pltpu.VMEM((keep, 8 * keep), F32),
            pltpu.VMEM(prior_t.shape, prior_t.dtype),
            pltpu.VMEM(frames.shape, frames.dtype),
        ),
        in_specs=[pl.BlockSpec(memory_space=pltpu.MemorySpace.HBM)] * 2,
        out_specs=[pl.BlockSpec(memory_space=VMEM)] * 4,
        scratch_shapes=[
            pltpu.SemaphoreType.DMA((2, len(cuts) - 1)),
            pltpu.VMEM((width + keep, width), F32),
            pltpu.VMEM((keep, keep), F32),
        ],
        name="gram",
        compiler_params=grant(GRAM_MB),
    )(prior_t, frames)


def split(value):
    high = value.astype(jnp.bfloat16)
    return high, (value - high.astype(F32)).astype(jnp.bfloat16)


def modes_kernel(first, weights_ref, prior_ref, frames_ref, out_ref):
    keep = prior_ref.shape[0]
    width = frames_ref.shape[1]
    rows = out_ref.shape[1]
    both = jnp.concatenate(split(weights_ref[:, : width + keep]), axis=0)
    size = block_of(rows, 2048)
    for at in range(0, rows, size):
        here = slice(first + at, first + at + size)
        whole = jnp.concatenate([frames_ref[here].T, prior_ref[:, here]], axis=0)
        part = fast(both, whole)
        out_ref[:, at : at + size] = (part[:keep] + part[keep:]).astype(out_ref.dtype)


def project(weights, prior_t, frames, first, rows):
    keep = prior_t.shape[0]
    return pl.pallas_call(
        functools.partial(modes_kernel, first),
        out_shape=pltpu.VMEM((keep, rows), jnp.bfloat16),
        in_specs=[pl.BlockSpec(memory_space=VMEM)] * 3,
        out_specs=pl.BlockSpec(memory_space=VMEM),
        name="project",
        compiler_params=grant(PROJ_MB),
    )(weights, prior_t, frames)


def pair_kernel(own_ref, other_ref, *rest):
    out_ref = rest[-1]
    half = out_ref.shape[0]
    gram = fast(own_ref[...], other_ref[...], NT)
    gram = jnp.concatenate([gram[:half], gram[half:]], axis=1)
    out_ref[...] = rest[0][...] + gram if len(rest) > 1 else gram


def pair_gram(own, other, *sofar):
    keep = own.shape[0]
    return pl.pallas_call(
        pair_kernel,
        out_shape=jax.ShapeDtypeStruct((keep // 2, 2 * keep), F32),
        in_specs=[pl.BlockSpec(memory_space=VMEM)] * (2 + len(sofar)),
        out_specs=pl.BlockSpec(memory_space=VMEM),
        name="pair",
        compiler_params=grant(PAIR_MB),
    )(own, other, *sofar)


def merge_kernel(left_ref, right_ref, own_ref, other_ref, out_ref, zero_ref):
    zero_ref[...] = jnp.zeros_like(zero_ref)
    keep = own_ref.shape[0]
    halves = left_ref[...] + right_ref[...]
    cross = jnp.concatenate([halves[:, :keep], halves[:, keep:]], axis=0)
    gram = jnp.concatenate(
        [
            jnp.concatenate([own_ref[...], cross], axis=1),
            jnp.concatenate([cross.T, other_ref[...]], axis=1),
        ],
        axis=0,
    )
    gram = gram * (1.0 / trace(gram))
    first = lax.axis_index("tm") == 0
    swapped = pltpu.roll(pltpu.roll(gram, keep, 1), keep, 0)
    basis = basis_rows(jnp.where(first, gram, swapped), keep, zero_ref[...])
    half = out_ref.shape[0]
    out_ref[...] = jnp.where(first, basis[:half], pltpu.roll(basis[half:], keep, 1))


def merge_weights(left, right, own, other):
    keep = own.shape[0]
    return pl.pallas_call(
        merge_kernel,
        out_shape=jax.ShapeDtypeStruct((keep // 2, 2 * keep), F32),
        in_specs=[pl.BlockSpec(memory_space=VMEM)] * 4,
        out_specs=pl.BlockSpec(memory_space=VMEM),
        scratch_shapes=[pltpu.VMEM((8, 2 * keep), F32)],
        name="merge",
        compiler_params=grant(2),
    )(left, right, own, other)


def output_kernel(pieces, weights_ref, *refs):
    owns, others = refs[:pieces], refs[pieces : 2 * pieces]
    out_ref, held_ref, sems = refs[2 * pieces :]
    half = out_ref.shape[0]
    weights = jnp.concatenate(split(weights_ref[...]), axis=0)
    rows = owns[0].shape[1]
    copies = []
    for i in range(pieces):
        both = jnp.concatenate([owns[i][...], others[i][...]], axis=0)
        part = fast(weights, both)
        here = slice(i * rows, i * rows + rows)
        held_ref[:, here] = (part[:half] + part[half:]).astype(out_ref.dtype)
        copies.append(pltpu.make_async_copy(held_ref.at[:, here], out_ref.at[:, here], sems.at[i]))
        copies[-1].start()
    for copy in copies:
        copy.wait()


def output(weights, owns, others):
    keep = owns[0].shape[0]
    rows = sum(own.shape[1] for own in owns)
    shape = (keep // 2, rows)
    return pl.pallas_call(
        functools.partial(output_kernel, len(owns)),
        out_shape=jax.ShapeDtypeStruct(shape, jnp.bfloat16),
        in_specs=[pl.BlockSpec(memory_space=VMEM)] * (1 + 2 * len(owns)),
        out_specs=pl.BlockSpec(memory_space=pltpu.MemorySpace.HBM),
        scratch_shapes=[pltpu.VMEM(shape, jnp.bfloat16), pltpu.SemaphoreType.DMA((len(owns),))],
        name="output",
        compiler_params=grant(OUT_MB),
    )(weights, *owns, *others)


def flip(block, axis, mask):
    count = lax.axis_size(axis)
    return lax.ppermute(block, axis, [(i, i ^ mask) for i in range(count)])


def all_but_last_sum(value, axis, mirror):
    count = lax.axis_size(axis)
    masks = [1 << bit for bit in range(count.bit_length() - 1)]
    if mirror:
        masks = masks[:1] + [2 * mask - 2 for mask in masks[1:]]
    for mask in masks[:-1]:
        value = value + flip(value, axis, mask)
    return value, flip(value, axis, masks[-1])


def cuts_of(rows):
    unit = rows // 32
    return [unit * at for at in (0, 1, 4, 12, 20, 28, 32)]


def block_of(rows, limit):
    size = min(rows, limit)
    while rows % size:
        size //= 2
    return size


def shards(prior, snapshots):
    keep = prior.shape[2]
    rows = prior.shape[1]
    early, late, prior_t, frames = local_gram(prior[0].T, snapshots[0], cuts_of(rows))
    early, late = (all_but_last_sum(part, "rows", True) for part in (early, late))
    weights, own_gram = steps_weights(early, late, keep)
    other_gram = flip(own_gram, "tm", 1)
    piece = rows // PIECES
    owns, others = [], []
    for i in range(PIECES):
        owns.append(project(weights, prior_t, frames, i * piece, piece))
        others.append(flip(owns[-1], "tm", 1))
    cross = pair_gram(owns[0], others[0])
    for own, other in zip(owns[1:], others[1:]):
        cross = pair_gram(own, other, cross)
    final = merge_weights(*all_but_last_sum(cross, "rows", False), own_gram, other_gram)
    return output(final, owns, others).T


def solution(mesh):
    in_specs = (P("tm", ("job", "rows"), None), P("tm", ("job", "rows"), None))
    out_specs = P(("job", "rows"), "tm")
    return jax.shard_map(shards, mesh=mesh, in_specs=in_specs, out_specs=out_specs, check_vma=False)
```

```python
import functools

import jax
import jax.numpy as jnp
from jax import lax
from jax.experimental import pallas as pl
from jax.experimental.pallas import tpu as pltpu
from jax.sharding import PartitionSpec as P

STEPS = 4
ITERS = 2
F32 = jnp.float32
NN = (((1,), (0,)), ((), ()))
NT = (((1,), (1,)), ((), ()))
TN = (((0,), (0,)), ((), ()))
VMEM = pltpu.MemorySpace.VMEM
EARLY = 2
STEPS_FLOPS = 10**10
PIECES = 4
AHEAD = 2
GRAM_MB, PROJ_MB, PAIR_MB, OUT_MB = 36, 12, 6, 8


def dot(a, b, dims=NN):
    return lax.dot_general(
        a, b, dims, precision=lax.Precision.HIGHEST, preferred_element_type=F32
    )


def fast(a, b, dims=NN):
    return lax.dot_general(a, b, dims, preferred_element_type=F32)


def spread_lanes(row):
    return jnp.broadcast_to(row, (8, row.shape[1]))


def spread_cols(col, width):
    return jnp.broadcast_to(col, (col.shape[0], width))


def grant(mebibytes):
    return pltpu.CompilerParams(vmem_limit_bytes=mebibytes << 20)


def iota(shape, dim):
    return lax.broadcasted_iota(jnp.int32, shape, dim)


def pair_sum(terms):
    while len(terms) > 1:
        terms = [a + b for a, b in zip(terms[::2], terms[1::2])]
    return terms[0]


def eliminate(here, cols):
    cols = list(cols)
    sub = iota(here.shape, 0)
    kept = here
    for j in range(0, 8, 2):
        left, right = cols[j], cols[j + 1]
        at_left, at_right = sub == j, sub == j + 1
        pp, pq, qq = (
            spread_lanes(left[j : j + 1]),
            spread_lanes(right[j : j + 1]),
            spread_lanes(right[j + 1 : j + 2]),
        )
        inv = 1.0 / (pp * qq - pq * pq)
        ipp, ipq, iqq = qq * inv, -pq * inv, pp * inv

        def solve(value):
            top, low = spread_lanes(value[j : j + 1]), spread_lanes(value[j + 1 : j + 2])
            up, down = ipp * top + ipq * low, ipq * top + iqq * low
            rest = value - (left * up + right * down)
            return top, low, jnp.where(at_left, up, jnp.where(at_right, down, rest))

        for k in range(j + 2, len(cols)):
            cols[k] = solve(cols[k])[2]
        top, low, here = solve(here)
        scale = lax.rsqrt(pp)
        ratio = pq * scale
        unit = top * scale
        kept = jnp.where(at_left, unit, kept)
        kept = jnp.where(at_right, (low - ratio * unit) * lax.rsqrt(qq - ratio * ratio), kept)
    return kept, here, cols


def subtract(value, cols, rows):
    return value - pair_sum([col * row for col, row in zip(cols, rows)])


def inverse_factor(square, zero):
    order, width = square.shape
    lane = iota((order, width), 1)
    eye = (lane == iota((order, width), 0)).astype(F32)
    joined = jnp.where(lane < order, eye, square)
    count = order // 8
    rows = [joined[8 * b : 8 * b + 8] for b in range(count)]

    def columns(row, first):
        return [
            spread_cols(row[:, first + j : first + j + 1], width) + zero for j in range(16)
        ]

    def spread_rows(value):
        return [spread_lanes(value[j : j + 1]) for j in range(8)]

    done = []
    for b in range(0, count, 2):
        first = order + 8 * b
        cols, low_cols = columns(rows[b], first), columns(rows[b + 1], first)
        below = [columns(rows[t], first) for t in range(b + 2, count)]
        kept, high, cols = eliminate(rows[b], cols)
        done.append(kept)
        low = subtract(rows[b + 1], low_cols[:8], spread_rows(high))
        next_cols = [
            subtract(low_cols[k], low_cols[:8], spread_rows(cols[k])) for k in range(8, 16)
        ]
        kept, low, _ = eliminate(low, next_cols)
        done.append(kept)
        if b + 2 < count:
            low_rows = spread_rows(low)
            high_rows = spread_rows(subtract(high, cols[8:], low_rows))
            for at, t in enumerate(range(b + 2, count)):
                rows[t] = subtract(rows[t], below[at], high_rows + low_rows)
    return jnp.where(lane < order, jnp.concatenate(done, axis=0), 0.0)


def basis_rows(gram, keep, zero):
    image = gram[:keep]
    for turn in range(ITERS):
        twice = jnp.concatenate([image, image], axis=0)
        inner = dot(image, twice, NT)
        basis = dot(inverse_factor(inner, zero), twice)
        if turn + 1 < ITERS:
            image = dot(basis, gram)
    return basis


def assemble(square, cross, corner):
    low = jnp.concatenate([cross, corner], axis=1)
    size = square.shape[0]
    pad = jnp.zeros((128 - cross.shape[0], size), F32)
    top = jnp.concatenate([square, jnp.concatenate([cross, pad], axis=0).T], axis=1)
    return jnp.concatenate([top, low, jnp.zeros_like(low)], axis=0)


def prior_block(mixed):
    keep = mixed.shape[0]
    lane, row = iota(mixed.shape, 1), iota(mixed.shape, 0)
    turned = jnp.concatenate([mixed, mixed], axis=0).T[:keep]
    return jnp.where(lane < keep, jnp.where(row <= lane, mixed, turned), 0.0)


def unpack_early(early):
    mixed = early[:, 256:384]
    upper = jnp.concatenate([early[:, 0:128], mixed], axis=0)
    square = jnp.where(iota(upper.shape, 0) <= iota(upper.shape, 1), upper, upper.T)
    return assemble(square, early[:, 128:256], prior_block(mixed))


def unpack(early, late):
    keep = early.shape[0]
    tile = lambda i: late[:, 128 * i : 128 * i + 128]
    lane, row = iota((keep, 128), 1), iota((keep, 128), 0)
    zero = jnp.zeros((keep, 128), F32)
    first, mixed = early[:, 0:128], early[:, 256:384]
    diag = jnp.where(
        lane == 127,
        pltpu.roll(jnp.broadcast_to(mixed[keep - 2 : keep - 1], mixed.shape), 127, 1),
        pltpu.roll(jnp.broadcast_to(mixed[keep - 1 : keep], mixed.shape), keep, 1),
    )
    end = jnp.where(lane == row + keep, diag, pltpu.roll(first, keep, 1))
    upper = jnp.concatenate(
        [
            jnp.concatenate([first, tile(0)], axis=1),
            jnp.concatenate([mixed, tile(1)], axis=1),
            jnp.concatenate([zero, tile(2)], axis=1),
            jnp.concatenate([zero, end], axis=1),
        ],
        axis=0,
    )
    size = upper.shape[0]
    high, wide = iota((size, size), 0), iota((size, size), 1)
    last = size - keep
    held = ((high <= wide) & (wide < last)) | ((high < last) & (wide >= last))
    held |= (high >= wide) & (high >= last) & (wide >= last)
    square = jnp.where(held, upper, upper.T)
    cross = jnp.concatenate([early[:, 128:256], tile(3)], axis=1)
    return assemble(square, cross, prior_block(mixed))


def trace(gram):
    return jnp.sum(jnp.where(iota(gram.shape, 0) == iota(gram.shape, 1), gram, 0.0))


def run_steps(first, last, keep, total_ref, both_ref, zero):
    width = total_ref.shape[0]
    shape = (keep, width)

    @pl.loop(first, last)
    def _(step):
        at = pl.multiple_of(step * keep, keep)
        both_ref[keep:, :width] = total_ref[pl.ds(at, keep)]
        both_ref[keep:, width:] = (iota(shape, 1) == iota(shape, 0) + at).astype(F32)
        both = both_ref[...]
        gram = dot(both[:, :width], both[:, width:], NT)
        both_ref[:keep] = dot(basis_rows(gram, keep, zero), both)


def early_kernel(left_ref, right_ref, out_ref, total_ref, both_ref, zero_ref):
    keep = left_ref.shape[0]
    zero_ref[...] = jnp.zeros_like(zero_ref)
    total = unpack_early(left_ref[...] + right_ref[...])
    total = total * (1.0 / trace(total))
    total_ref[...] = total
    width = total.shape[0]
    frames = EARLY * keep
    shape = (keep, width)
    both_ref[:keep, :width] = total[frames : frames + keep]
    both_ref[:keep, width:] = (iota(shape, 1) == iota(shape, 0) + frames).astype(F32)
    run_steps(0, EARLY, keep, total_ref, both_ref, zero_ref[...])
    out_ref[...] = both_ref[:keep, width:]


def late_kernel(
    left_ref, right_ref, late_left, late_right, before_ref, out_ref, modes_ref, total_ref, both_ref, zero_ref
):
    keep = left_ref.shape[0]
    zero_ref[...] = jnp.zeros_like(zero_ref)
    total = unpack(left_ref[...] + right_ref[...], late_left[...] + late_right[...])
    scale = trace(total)
    total = total * (1.0 / scale)
    total_ref[...] = total
    width = total.shape[0]
    before = before_ref[...]
    fresh = EARLY * keep
    gap = jnp.zeros((keep, (STEPS - EARLY) * keep), F32)
    weights = jnp.concatenate([before[:, :fresh], gap, before[:, fresh:]], axis=1)
    both_ref[:keep, :width] = dot(weights, total)
    both_ref[:keep, width:] = weights
    run_steps(EARLY, STEPS, keep, total_ref, both_ref, zero_ref[...])
    out_ref[...] = both_ref[:keep, width:]
    modes_ref[...] = dot(both_ref[:keep, :width], both_ref[:keep, width:], NT) * scale


def steps_weights(early, late, keep):
    def call(kernel, shapes, width, *args):
        return pl.pallas_call(
            kernel,
            out_shape=tuple(jax.ShapeDtypeStruct(shape, F32) for shape in shapes),
            in_specs=[pl.BlockSpec(memory_space=VMEM)] * len(args),
            out_specs=tuple(pl.BlockSpec(memory_space=VMEM) for shape in shapes),
            scratch_shapes=[
                pltpu.VMEM((width, width), F32),
                pltpu.VMEM((2 * keep, 2 * width), F32),
                pltpu.VMEM((8, 2 * keep), F32),
            ],
            name="steps",
            compiler_params=grant(6),
            cost_estimate=pl.CostEstimate(
                flops=STEPS_FLOPS, bytes_accessed=1 << 20, transcendentals=0
            ),
        )(*args)

    (before,) = call(early_kernel, [(keep, (EARLY + 2) * keep)], (EARLY + 2) * keep, *early)
    width = (STEPS + 2) * keep
    return call(late_kernel, [(keep, width), (keep, keep)], width, *early, *late, before)


def gram_kernel(
    cuts, prior_in, frames_in, early_ref, late_ref, prior_ref, frames_ref, sems, square_ref, corner_ref
):
    keep = prior_ref.shape[0]
    blocks = [slice(low, high) for low, high in zip(cuts[:-1], cuts[1:])]

    def copies(i):
        at = blocks[i]
        return (
            pltpu.make_async_copy(prior_in.at[:, at], prior_ref.at[:, at], sems.at[0, i]),
            pltpu.make_async_copy(frames_in.at[at], frames_ref.at[at], sems.at[1, i]),
        )

    for i in range(min(AHEAD, len(blocks))):
        for copy in copies(i):
            copy.start()
    for i, at in enumerate(blocks):
        for copy in copies(i):
            copy.wait()
        if i + AHEAD < len(blocks):
            for copy in copies(i + AHEAD):
                copy.start()
        frames = frames_ref[at]
        prior = prior_ref[:, at]
        part = jnp.concatenate([fast(frames, frames, TN), fast(prior, frames)], axis=0)
        last = fast(prior, prior, NT)
        square_ref[...] = part if i == 0 else square_ref[...] + part
        corner_ref[...] = last if i == 0 else corner_ref[...] + last

    corner = corner_ref[...]
    wide = jnp.concatenate([corner, jnp.zeros_like(corner)], axis=1)
    lane, row = iota(wide.shape, 1), iota(wide.shape, 0)
    end = square_ref[192:256, 128:256]
    diag = jnp.sum(jnp.where(lane == row + keep, end, 0.0), axis=0, keepdims=True)
    diag = jnp.broadcast_to(diag, end.shape)
    mixed = jnp.where(lane < keep, wide, square_ref[64:128, 0:128])
    mixed = jnp.where((row == keep - 1) & (lane < keep - 1), pltpu.roll(diag, keep, 1), mixed)
    mixed = jnp.where((row == keep - 2) & (lane == 0), pltpu.roll(diag, 1, 1), mixed)
    free = (lane < keep) & (row > lane)
    early_ref[:, 0:128] = jnp.where(free, pltpu.roll(end, keep, 1), square_ref[0:64, 0:128])
    early_ref[:, 128:256] = square_ref[256:320, 0:128]
    early_ref[:, 256:384] = mixed
    late_ref[:, 0:128] = square_ref[0:64, 128:256]
    late_ref[:, 128:256] = square_ref[64:128, 128:256]
    late_ref[:, 256:384] = square_ref[128:192, 128:256]
    late_ref[:, 384:512] = square_ref[256:320, 128:256]


def local_gram(prior_t, frames, cuts):
    keep, rows = prior_t.shape
    width = frames.shape[1]
    return pl.pallas_call(
        functools.partial(gram_kernel, cuts),
        out_shape=(
            pltpu.VMEM((keep, 6 * keep), F32),
            pltpu.VMEM((keep, 8 * keep), F32),
            pltpu.VMEM(prior_t.shape, prior_t.dtype),
            pltpu.VMEM(frames.shape, frames.dtype),
        ),
        in_specs=[pl.BlockSpec(memory_space=pltpu.MemorySpace.HBM)] * 2,
        out_specs=[pl.BlockSpec(memory_space=VMEM)] * 4,
        scratch_shapes=[
            pltpu.SemaphoreType.DMA((2, len(cuts) - 1)),
            pltpu.VMEM((width + keep, width), F32),
            pltpu.VMEM((keep, keep), F32),
        ],
        name="gram",
        compiler_params=grant(GRAM_MB),
    )(prior_t, frames)


def split(value):
    high = value.astype(jnp.bfloat16)
    return high, (value - high.astype(F32)).astype(jnp.bfloat16)


def modes_kernel(first, weights_ref, prior_ref, frames_ref, out_ref):
    keep = prior_ref.shape[0]
    width = frames_ref.shape[1]
    rows = out_ref.shape[1]
    both = jnp.concatenate(split(weights_ref[:, : width + keep]), axis=0)
    size = block_of(rows, 2048)
    for at in range(0, rows, size):
        here = slice(first + at, first + at + size)
        whole = jnp.concatenate([frames_ref[here].T, prior_ref[:, here]], axis=0)
        part = fast(both, whole)
        out_ref[:, at : at + size] = (part[:keep] + part[keep:]).astype(out_ref.dtype)


def project(weights, prior_t, frames, first, rows):
    keep = prior_t.shape[0]
    return pl.pallas_call(
        functools.partial(modes_kernel, first),
        out_shape=pltpu.VMEM((keep, rows), jnp.bfloat16),
        in_specs=[pl.BlockSpec(memory_space=VMEM)] * 3,
        out_specs=pl.BlockSpec(memory_space=VMEM),
        name="project",
        compiler_params=grant(PROJ_MB),
    )(weights, prior_t, frames)


def pair_kernel(own_ref, other_ref, *rest):
    out_ref = rest[-1]
    half = out_ref.shape[0]
    gram = fast(own_ref[...], other_ref[...], NT)
    gram = jnp.concatenate([gram[:half], gram[half:]], axis=1)
    out_ref[...] = rest[0][...] + gram if len(rest) > 1 else gram


def pair_gram(own, other, *sofar):
    keep = own.shape[0]
    return pl.pallas_call(
        pair_kernel,
        out_shape=jax.ShapeDtypeStruct((keep // 2, 2 * keep), F32),
        in_specs=[pl.BlockSpec(memory_space=VMEM)] * (2 + len(sofar)),
        out_specs=pl.BlockSpec(memory_space=VMEM),
        name="pair",
        compiler_params=grant(PAIR_MB),
    )(own, other, *sofar)


def merge_kernel(left_ref, right_ref, own_ref, other_ref, out_ref, zero_ref):
    zero_ref[...] = jnp.zeros_like(zero_ref)
    keep = own_ref.shape[0]
    halves = left_ref[...] + right_ref[...]
    cross = jnp.concatenate([halves[:, :keep], halves[:, keep:]], axis=0)
    gram = jnp.concatenate(
        [
            jnp.concatenate([own_ref[...], cross], axis=1),
            jnp.concatenate([cross.T, other_ref[...]], axis=1),
        ],
        axis=0,
    )
    gram = gram * (1.0 / trace(gram))
    first = lax.axis_index("tm") == 0
    swapped = pltpu.roll(pltpu.roll(gram, keep, 1), keep, 0)
    basis = basis_rows(jnp.where(first, gram, swapped), keep, zero_ref[...])
    half = out_ref.shape[0]
    out_ref[...] = jnp.where(first, basis[:half], pltpu.roll(basis[half:], keep, 1))


def merge_weights(left, right, own, other):
    keep = own.shape[0]
    return pl.pallas_call(
        merge_kernel,
        out_shape=jax.ShapeDtypeStruct((keep // 2, 2 * keep), F32),
        in_specs=[pl.BlockSpec(memory_space=VMEM)] * 4,
        out_specs=pl.BlockSpec(memory_space=VMEM),
        scratch_shapes=[pltpu.VMEM((8, 2 * keep), F32)],
        name="merge",
        compiler_params=grant(2),
    )(left, right, own, other)


def output_kernel(pieces, weights_ref, *refs):
    owns, others = refs[:pieces], refs[pieces : 2 * pieces]
    out_ref, held_ref, sems = refs[2 * pieces :]
    half = out_ref.shape[0]
    weights = jnp.concatenate(split(weights_ref[...]), axis=0)
    rows = owns[0].shape[1]
    copies = []
    for i in range(pieces):
        both = jnp.concatenate([owns[i][...], others[i][...]], axis=0)
        part = fast(weights, both)
        here = slice(i * rows, i * rows + rows)
        held_ref[:, here] = (part[:half] + part[half:]).astype(out_ref.dtype)
        copies.append(pltpu.make_async_copy(held_ref.at[:, here], out_ref.at[:, here], sems.at[i]))
        copies[-1].start()
    for copy in copies:
        copy.wait()


def output(weights, owns, others):
    keep = owns[0].shape[0]
    rows = sum(own.shape[1] for own in owns)
    shape = (keep // 2, rows)
    return pl.pallas_call(
        functools.partial(output_kernel, len(owns)),
        out_shape=jax.ShapeDtypeStruct(shape, jnp.bfloat16),
        in_specs=[pl.BlockSpec(memory_space=VMEM)] * (1 + 2 * len(owns)),
        out_specs=pl.BlockSpec(memory_space=pltpu.MemorySpace.HBM),
        scratch_shapes=[pltpu.VMEM(shape, jnp.bfloat16), pltpu.SemaphoreType.DMA((len(owns),))],
        name="output",
        compiler_params=grant(OUT_MB),
    )(weights, *owns, *others)


def flip(block, axis, mask):
    count = lax.axis_size(axis)
    return lax.ppermute(block, axis, [(i, i ^ mask) for i in range(count)])


def hop(block, masks):
    count = lax.axis_size("rows")
    route = [
        (t * count + i, t * count + (i ^ mask)) for t, mask in enumerate(masks) for i in range(count)
    ]
    return lax.ppermute(block, ("tm", "rows"), route)


def all_but_last_sum(value, mirror):
    bits = lax.axis_size("rows").bit_length() - 1
    masks = [1 << bit for bit in range(bits)]
    if mirror:
        masks = masks[:1] + [2 * mask - 2 for mask in masks[1:]]
    hops = [
        [masks[(at + t) % bits] for t in range(lax.axis_size("tm"))] for at in range(bits)
    ]
    for step in hops[:-1]:
        value = value + hop(value, step)
    return value, hop(value, hops[-1])


def cuts_of(rows):
    unit = rows // 32
    return [unit * at for at in (0, 1, 4, 12, 20, 28, 32)]


def block_of(rows, limit):
    size = min(rows, limit)
    while rows % size:
        size //= 2
    return size


def shards(prior, snapshots):
    keep = prior.shape[2]
    rows = prior.shape[1]
    early, late, prior_t, frames = local_gram(prior[0].T, snapshots[0], cuts_of(rows))
    early, late = (all_but_last_sum(part, True) for part in (early, late))
    weights, own_gram = steps_weights(early, late, keep)
    other_gram = flip(own_gram, "tm", 1)
    piece = rows // PIECES
    owns, others = [], []
    for i in range(PIECES):
        owns.append(project(weights, prior_t, frames, i * piece, piece))
        others.append(flip(owns[-1], "tm", 1))
    cross = pair_gram(owns[0], others[0])
    for own, other in zip(owns[1:], others[1:]):
        cross = pair_gram(own, other, cross)
    final = merge_weights(*all_but_last_sum(cross, False), own_gram, other_gram)
    return output(final, owns, others).T


def solution(mesh):
    in_specs = (P("tm", ("job", "rows"), None), P("tm", ("job", "rows"), None))
    out_specs = P(("job", "rows"), "tm")
    return jax.shard_map(shards, mesh=mesh, in_specs=in_specs, out_specs=out_specs, check_vma=False)
```
